16 devices in a mesh: replica: 2 (over y, z), data: 8 (over x, core).
Axes of the slice: x: 4, y: 2, z: 1, core: 2. Of those that a mesh axis runs over, the one named last changes fastest.
The devices are a block of a 4x4x8 slice.
Arguments:
- q_hidden: bfloat16 [256, 32, 1024], P(('replica', 'data')), parts along dimension 0
- d_hidden: bfloat16 [256, 512, 1024], P(('replica', 'data')), parts along dimension 0
- w_proj: bfloat16 [1024, 128], replicated
- q_mask: int32 [256, 32], P(('replica', 'data')), parts along dimension 0
- d_mask: int32 [256, 512], P(('replica', 'data')), parts along dimension 0
- temperature: float32 [], replicated
Outputs:
- output 1: float32 [256], P(('replica', 'data')), parts along dimension 0
- output 2: float32 [256], P(('replica', 'data')), parts along dimension 0
- output 3: float32 [2], P('replica'), parts along dimension 0
There are 2 independent parts. The reference program is written for one: setup_inputs(seed, part) draws one part's arguments, and reference() takes and returns one part's arrays. A program takes and returns all parts, laid end to end along the dimension named above; an argument that names none is the same for every part.
All inputs are finite; a program needn't handle non-finite values.
Results may differ from the reference program's by a relative error of at most 0.001.
Values are sent between devices in bfloat16 or wider.
A program may use at most 768 MiB of HBM per device.

```python
import jax
import jax.numpy as jnp
from jax import lax

HIDDEN = 1024
PROJ_DIM = 128
Q_LEN = 32
DOC_LEN = 512
GROUP_PAIRS = 128


def setup_inputs(seed: int = 0, part: int = 0) -> dict:
    root_key = jax.random.key(seed)
    shared_keys = jax.random.split(jax.random.fold_in(root_key, 1), 2)
    part_keys = jax.random.split(jax.random.fold_in(jax.random.fold_in(root_key, 2), part), 6)
    w_proj = jax.random.normal(shared_keys[0], (HIDDEN, PROJ_DIM), jnp.float32) * HIDDEN ** -0.5
    temperature = jax.random.uniform(shared_keys[1], (), jnp.float32, 0.12, 0.2) * Q_LEN
    common = jax.random.normal(part_keys[0], (HIDDEN,), jnp.float32)
    topics = jax.random.normal(part_keys[1], (GROUP_PAIRS, HIDDEN), jnp.float32)
    q_noise = jax.random.normal(part_keys[2], (GROUP_PAIRS, Q_LEN, HIDDEN), jnp.float32)
    d_noise = jax.random.normal(part_keys[3], (GROUP_PAIRS, DOC_LEN, HIDDEN), jnp.float32)
    q_lens = jax.random.randint(part_keys[4], (GROUP_PAIRS,), Q_LEN // 2, Q_LEN + 1)
    d_lens = jax.random.randint(part_keys[5], (GROUP_PAIRS,), DOC_LEN // 4, DOC_LEN + 1)
    q_mask = (jnp.arange(Q_LEN)[None, :] < q_lens[:, None]).astype(jnp.int32)
    d_mask = (jnp.arange(DOC_LEN)[None, :] < d_lens[:, None]).astype(jnp.int32)
    q_real = common + topics[:, None, :] + q_noise
    q_pad = common + 2.0 * jnp.roll(topics, 1, axis=0)[:, None, :] + 0.5 * q_noise
    d_real = common + topics[:, None, :] + d_noise
    d_pad = 4.0 * common + 0.5 * d_noise
    q_hidden = jnp.where(q_mask[:, :, None] == 1, q_real, q_pad).astype(jnp.bfloat16)
    d_hidden = jnp.where(d_mask[:, :, None] == 1, d_real, d_pad).astype(jnp.bfloat16)
    return {'q_hidden': q_hidden, 'd_hidden': d_hidden, 'w_proj': w_proj.astype(jnp.bfloat16), 'q_mask': q_mask, 'd_mask': d_mask, 'temperature': temperature}


def project(hidden, w_proj):
    flat_rows = hidden.reshape(-1, hidden.shape[-1])
    raw_proj = jnp.dot(flat_rows, w_proj, preferred_element_type=jnp.float32)
    unit_vecs = raw_proj / jnp.sqrt(jnp.sum(raw_proj * raw_proj, axis=-1, keepdims=True))
    return unit_vecs.astype(jnp.bfloat16).reshape(hidden.shape[:-1] + (w_proj.shape[1],))


def reference(q_hidden, d_hidden, w_proj, q_mask, d_mask, temperature):
    q_vecs = project(q_hidden, w_proj).astype(jnp.float32)
    p_vecs = project(d_hidden, w_proj).astype(jnp.float32)
    doc_valid = d_mask == 1

    def score_row(row_args):
        q_row, q_valid = row_args
        sim_vals = jnp.einsum('tk,jsk->tjs', q_row, p_vecs)
        best_sim = jnp.max(jnp.where(doc_valid[None, :, :], sim_vals, -jnp.inf), axis=2)
        return jnp.sum(jnp.where(q_valid[:, None] == 1, best_sim, 0.0), axis=0)

    scores = lax.map(score_row, (q_vecs, q_mask))
    logits = scores / temperature
    pos_logit = jnp.diagonal(logits)
    loss_query = jax.nn.logsumexp(logits, axis=1) - pos_logit
    loss_doc = jax.nn.logsumexp(logits, axis=0) - pos_logit
    loss_mean = (0.5 * jnp.mean(loss_query + loss_doc)).reshape(1)
    return loss_query, loss_doc, loss_mean
```

```python
import functools
import jax
import jax.numpy as jnp
from jax import lax
from jax.experimental import pallas as pl
from jax.experimental.pallas import tpu as pltpu
from jax.sharding import PartitionSpec as P

MESH = pl.DeviceIdType.MESH
NT = (((1,), (1,)), ((), ()))


def unit_rows(x):
    return x * lax.rsqrt(jnp.sum(x * x, axis=1, keepdims=True))


def kernel(dims, q_hbm, d_hbm, w_hbm, qm_hbm, dm_hbm, temp_ref, lq_ref, ld_ref, lm_ref,
           w, qh, dh, qm, dm, qall, u, dmt, s_all,
           in_sem, d_sem, q_send, q_recv, s_send, s_recv):
    n, pairs, q_len, d_len, gran = dims
    q_rows = pairs * q_len
    me = lax.axis_index('data')
    core = lax.rem(me, 2)
    chip = me // 2
    chips = n // 2
    partner = chip * 2 + (1 - core)

    def dev(dc, other):
        c = lax.rem(chip + dc, chips)
        return c * 2 + ((1 - core) if other else core)

    barrier = pltpu.get_barrier_semaphore()
    for o in range(1, n):
        pl.semaphore_signal(barrier, inc=1, device_id={'data': lax.rem(me + o, n)}, device_id_type=MESH)

    ins = [pltpu.make_async_copy(src, dst, in_sem.at[i]) for i, (src, dst) in enumerate(
        ((w_hbm, w), (q_hbm, qh), (qm_hbm, qm), (dm_hbm, dm)))]
    for c in ins:
        c.start()
    grows = gran * d_len
    n_gran = pairs // gran
    d_copies = []
    for g in range(n_gran):
        c = pltpu.make_async_copy(d_hbm.at[pl.ds(g * grows, grows)], dh.at[pl.ds(g * grows, grows)], d_sem.at[g])
        c.start()
        d_copies.append(c)

    for c in ins:
        c.wait()

    row = lax.broadcasted_iota(jnp.int32, (q_rows, pairs), 0)
    own = (row // q_len == lax.broadcasted_iota(jnp.int32, (q_rows, pairs), 1)).astype(jnp.bfloat16)
    spread = jnp.dot(own, qm[...].astype(jnp.bfloat16), preferred_element_type=jnp.float32)
    row = lax.broadcasted_iota(jnp.int32, (q_rows, q_len), 0)
    tok = lax.broadcasted_iota(jnp.int32, (q_rows, q_len), 1)
    q_keep = jnp.sum(jnp.where(row % q_len == tok, spread, 0.0), axis=1, keepdims=True)
    xq = unit_rows(jnp.dot(qh[...], w[...], preferred_element_type=jnp.float32))
    qall[me] = jnp.where(q_keep > 0.5, xq, 0.0).astype(jnp.bfloat16)

    dmf = dm[...].astype(jnp.float32)
    dmt[...] = dmf.T
    pos = lax.broadcasted_iota(jnp.int32, (pairs, d_len), 1).astype(jnp.float32)
    first = jnp.min(jnp.where(dmf > 0.5, pos, float(d_len)), axis=1, keepdims=True)

    pl.semaphore_wait(barrier, n - 1)

    def send(slot, target, i):
        c = pltpu.make_async_remote_copy(
            src_ref=qall.at[slot], dst_ref=qall.at[slot], send_sem=q_send.at[i], recv_sem=q_recv.at[slot],
            device_id={'data': target}, device_id_type=MESH)
        c.start()
        return c

    def arrive(slot):
        pltpu.make_async_remote_copy(
            src_ref=qall.at[slot], dst_ref=qall.at[slot], send_sem=q_send.at[0], recv_sem=q_recv.at[slot],
            device_id={'data': partner}, device_id_type=MESH).wait_recv()

    hops = [1, chips - 1] + list(range(2, chips - 1))
    sends = [send(me, dev(h, False), i) for i, h in enumerate(hops)]
    sends.append(send(me, partner, len(hops)))

    def project(g):
        x = unit_rows(jnp.dot(dh[pl.ds(g * grows, grows), :], w[...], preferred_element_type=jnp.float32))
        for k in range(gran):
            j = g * gran + k
            xj = x[k * d_len:(k + 1) * d_len]
            at = lax.broadcasted_iota(jnp.int32, (d_len, 1), 0).astype(jnp.float32)
            rep = jnp.sum(jnp.where(at == first[j:j + 1, :], xj, 0.0), axis=0, keepdims=True)
            keep = dmt[:, j:j + 1] > 0.5
            u[pl.ds(j * d_len, d_len), :] = jnp.where(keep, xj, rep).astype(jnp.bfloat16)

    def best_of(slot, j):
        sim = lax.dot_general(u[pl.ds(j * d_len, d_len), :], qall[slot], NT, preferred_element_type=jnp.float32)
        return jnp.max(sim, axis=0, keepdims=True)

    sel = (lax.broadcasted_iota(jnp.int32, (q_rows, 128), 0) // q_len
           == lax.broadcasted_iota(jnp.int32, (q_rows, 128), 1)).astype(jnp.bfloat16)

    def scores(slot, rows):
        best = jnp.concatenate(rows, axis=0)
        hi = best.astype(jnp.bfloat16)
        r1 = best - hi.astype(jnp.float32)
        mid = r1.astype(jnp.bfloat16)
        lo = (r1 - mid.astype(jnp.float32)).astype(jnp.bfloat16)
        s = jnp.dot(hi, sel, preferred_element_type=jnp.float32)
        s = s + (jnp.dot(mid, sel, preferred_element_type=jnp.float32)
                 + jnp.dot(lo, sel, preferred_element_type=jnp.float32))
        return pltpu.roll(s, slot * pairs, 1)

    rows = []
    for g in range(n_gran):
        d_copies[g].wait()
        project(g)
        if g > 0:
            rows += [best_of(me, (g - 1) * gran + k) for k in range(gran)]
    rows += [best_of(me, (n_gran - 1) * gran + k) for k in range(gran)]
    total = scores(me, rows)

    def forward(h, i):
        slot = dev(h, False)
        arrive(slot)
        sends.append(send(slot, partner, i))

    forward(hops[0], n - chips + 0)
    forward(hops[1], n - chips + 1)
    arrive(partner)
    total += scores(partner, [best_of(partner, j) for j in range(pairs)])
    slot = dev(hops[0], False)
    total += scores(slot, [best_of(slot, j) for j in range(pairs)])
    slot = dev(hops[1], False)
    total += scores(slot, [best_of(slot, j) for j in range(pairs)])
    for i, h in enumerate(hops[2:]):
        forward(h, n - chips + 2 + i)
    for h in hops[:2]:
        slot = dev(h, True)
        arrive(slot)
        total += scores(slot, [best_of(slot, j) for j in range(pairs)])
    for h in hops[2:]:
        slot = dev(h, False)
        total += scores(slot, [best_of(slot, j) for j in range(pairs)])
    for h in hops[2:]:
        slot = dev(h, True)
        arrive(slot)
        total += scores(slot, [best_of(slot, j) for j in range(pairs)])

    mine = pl.ds(pl.multiple_of(me * pairs, pairs), pairs)
    s_all[mine, :] = total
    s_sends = []
    for o in range(1, n):
        c = pltpu.make_async_remote_copy(
            src_ref=s_all.at[mine], dst_ref=s_all.at[mine], send_sem=s_send.at[o], recv_sem=s_recv.at[me],
            device_id={'data': lax.rem(me + o, n)}, device_id_type=MESH)
        c.start()
        s_sends.append(c)
    for c in sends:
        c.wait_send()
    for o in range(1, n):
        src = lax.rem(me + o, n)
        theirs = pl.ds(pl.multiple_of(src * pairs, pairs), pairs)
        pltpu.make_async_remote_copy(
            src_ref=s_all.at[theirs], dst_ref=s_all.at[theirs], send_sem=s_send.at[o], recv_sem=s_recv.at[src],
            device_id={'data': src}, device_id_type=MESH).wait_recv()
    for c in s_sends:
        c.wait_send()

    z = s_all[...] / temp_ref[0]
    size = n * pairs
    diag = (lax.broadcasted_iota(jnp.int32, (size, size), 0) == lax.broadcasted_iota(jnp.int32, (size, size), 1))
    pos_logit = jnp.sum(jnp.where(diag, z, 0.0), axis=0, keepdims=True)

    def lse(v):
        top = jnp.max(v, axis=0, keepdims=True)
        return jnp.log(jnp.sum(jnp.exp(v - top), axis=0, keepdims=True)) + top

    loss_q = lse(z) - pos_logit
    loss_d = lse(z.T) - pos_logit
    lm_ref[0] = jnp.sum(loss_q + loss_d) / (2 * size)
    back = lax.rem(size - me * pairs, size)
    lq_ref[...] = pltpu.roll(loss_q, back, 1)[:, :pairs]
    ld_ref[...] = pltpu.roll(loss_d, back, 1)[:, :pairs]


def solution(mesh):
    n = mesh.shape['data']
    batch_spec = P(('replica', 'data'))

    def local_loss(q_hidden, d_hidden, w_proj, q_mask, d_mask, temperature):
        pairs, q_len, hidden = q_hidden.shape
        d_len = d_hidden.shape[1]
        k = w_proj.shape[1]
        gran = 2
        any_ = pl.BlockSpec(memory_space=pl.ANY)
        lq, ld, lm = pl.pallas_call(
            functools.partial(kernel, (n, pairs, q_len, d_len, gran)),
            out_shape=(jax.ShapeDtypeStruct((1, pairs), jnp.float32), jax.ShapeDtypeStruct((1, pairs), jnp.float32),
                       jax.ShapeDtypeStruct((1,), jnp.float32)),
            in_specs=[any_] * 5 + [pl.BlockSpec(memory_space=pltpu.SMEM)],
            out_specs=(pl.BlockSpec(memory_space=pltpu.VMEM), pl.BlockSpec(memory_space=pltpu.VMEM),
                       pl.BlockSpec(memory_space=pltpu.SMEM)),
            scratch_shapes=[
                pltpu.VMEM((hidden, k), jnp.bfloat16),
                pltpu.VMEM((pairs * q_len, hidden), jnp.bfloat16),
                pltpu.VMEM((pairs * d_len, hidden), jnp.bfloat16),
                pltpu.VMEM((pairs, q_len), jnp.int32),
                pltpu.VMEM((pairs, d_len), jnp.int32),
                pltpu.VMEM((n, pairs * q_len, k), jnp.bfloat16),
                pltpu.VMEM((pairs * d_len, k), jnp.bfloat16),
                pltpu.VMEM((d_len, pairs), jnp.float32),
                pltpu.VMEM((n * pairs, n * pairs), jnp.float32),
                pltpu.SemaphoreType.DMA((4,)),
                pltpu.SemaphoreType.DMA((pairs // gran,)),
                pltpu.SemaphoreType.DMA((n,)),
                pltpu.SemaphoreType.DMA((n,)),
                pltpu.SemaphoreType.DMA((n,)),
                pltpu.SemaphoreType.DMA((n,)),
            ],
            compiler_params=pltpu.CompilerParams(
                collective_id=0, has_side_effects=True),
        )(q_hidden.reshape(pairs * q_len, hidden), d_hidden.reshape(pairs * d_len, hidden), w_proj,
          q_mask, d_mask, temperature.reshape(1))
        return lq.reshape(pairs), ld.reshape(pairs), lm

    return jax.shard_map(local_loss, mesh=mesh, in_specs=(batch_spec, batch_spec, P(), batch_spec, batch_spec, P()),
                         out_specs=(batch_spec, batch_spec, P('replica')), check_vma=False)
```

```python
import functools
import jax
import jax.numpy as jnp
from jax import lax
from jax.experimental import pallas as pl
from jax.experimental.pallas import tpu as pltpu
from jax.sharding import PartitionSpec as P

MESH = pl.DeviceIdType.MESH


def unit_rows(x):
    return x * lax.rsqrt(jnp.sum(x * x, axis=1, keepdims=True))


def kernel(dims, q_hbm, d_hbm, w_hbm, qm_hbm, dm_hbm, s_all,
           w, qh, dh, qm, dm, qall, u, dmt,
           in_sem, d_sem, q_send, q_recv, s_send, s_recv):
    n, pairs, q_len, d_len, gran = dims
    q_rows = pairs * q_len
    me = lax.axis_index('data')
    core = lax.rem(me, 2)
    chip = me // 2
    chips = n // 2
    partner = chip * 2 + (1 - core)

    def dev(dc, other):
        c = lax.rem(chip + dc, chips)
        return c * 2 + ((1 - core) if other else core)

    barrier = pltpu.get_barrier_semaphore()
    for o in range(1, n):
        pl.semaphore_signal(barrier, inc=1, device_id={'data': lax.rem(me + o, n)}, device_id_type=MESH)

    ins = [pltpu.make_async_copy(src, dst, in_sem.at[i]) for i, (src, dst) in enumerate(
        ((w_hbm, w), (q_hbm, qh), (qm_hbm, qm), (dm_hbm, dm)))]
    for c in ins:
        c.start()
    grows = gran * d_len
    n_gran = pairs // gran
    d_copies = []
    for g in range(n_gran):
        c = pltpu.make_async_copy(d_hbm.at[pl.ds(g * grows, grows)], dh.at[pl.ds(g * grows, grows)], d_sem.at[g])
        d_copies.append(c)
    for c in d_copies[:2]:
        c.start()

    for c in ins:
        c.wait()

    row = lax.broadcasted_iota(jnp.int32, (q_rows, pairs), 0)
    own = (row // q_len == lax.broadcasted_iota(jnp.int32, (q_rows, pairs), 1)).astype(jnp.bfloat16)
    spread = jnp.dot(own, qm[...].astype(jnp.bfloat16), preferred_element_type=jnp.float32)
    row = lax.broadcasted_iota(jnp.int32, (q_rows, q_len), 0)
    tok = lax.broadcasted_iota(jnp.int32, (q_rows, q_len), 1)
    q_keep = jnp.sum(jnp.where(row % q_len == tok, spread, 0.0), axis=1, keepdims=True)
    xq = unit_rows(jnp.dot(qh[...], w[...], preferred_element_type=jnp.float32))
    qall[me] = jnp.where(q_keep > 0.5, xq, 0.0).T.astype(jnp.bfloat16)

    dmf = dm[...].astype(jnp.float32)
    dmt[...] = dmf.T
    pos = lax.broadcasted_iota(jnp.int32, (pairs, d_len), 1).astype(jnp.float32)
    first = jnp.min(jnp.where(dmf > 0.5, pos, float(d_len)), axis=1, keepdims=True)

    def send(slot, target, i):
        c = pltpu.make_async_remote_copy(
            src_ref=qall.at[slot], dst_ref=qall.at[slot], send_sem=q_send.at[i], recv_sem=q_recv.at[slot],
            device_id={'data': target}, device_id_type=MESH)
        c.start()
        return c

    def arrive(slot):
        pltpu.make_async_remote_copy(
            src_ref=qall.at[slot], dst_ref=qall.at[slot], send_sem=q_send.at[0], recv_sem=q_recv.at[slot],
            device_id={'data': partner}, device_id_type=MESH).wait_recv()

    hops = [1, chips - 1] + list(range(2, chips - 1))
    sends = []

    def project(g):
        x = unit_rows(jnp.dot(dh[pl.ds(g * grows, grows), :], w[...], preferred_element_type=jnp.float32))
        for k in range(gran):
            j = g * gran + k
            xj = x[k * d_len:(k + 1) * d_len]
            at = lax.broadcasted_iota(jnp.int32, (d_len, 1), 0).astype(jnp.float32)
            rep = jnp.sum(jnp.where(at == first[j:j + 1, :], xj, 0.0), axis=0, keepdims=True)
            keep = dmt[:, j:j + 1] > 0.5
            u[pl.ds(j * d_len, d_len), :] = jnp.where(keep, xj, rep).astype(jnp.bfloat16)

    def best_of(slot, j):
        sim = jnp.dot(u[pl.ds(j * d_len, d_len), :], qall[slot], preferred_element_type=jnp.float32)
        return jnp.max(sim, axis=0, keepdims=True)

    sel = (lax.broadcasted_iota(jnp.int32, (q_rows, 128), 0) // q_len
           == lax.broadcasted_iota(jnp.int32, (q_rows, 128), 1)).astype(jnp.bfloat16)

    def scores(slot, rows):
        best = jnp.concatenate(rows, axis=0)
        hi = best.astype(jnp.bfloat16)
        r1 = best - hi.astype(jnp.float32)
        mid = r1.astype(jnp.bfloat16)
        lo = (r1 - mid.astype(jnp.float32)).astype(jnp.bfloat16)
        s = jnp.dot(hi, sel, preferred_element_type=jnp.float32)
        s = s + (jnp.dot(mid, sel, preferred_element_type=jnp.float32)
                 + jnp.dot(lo, sel, preferred_element_type=jnp.float32))
        return pltpu.roll(s, slot * pairs, 1)

    rows = []
    for g in range(n_gran):
        d_copies[g].wait()
        if g + 2 < n_gran:
            d_copies[g + 2].start()
        project(g)
        if g == 0:
            pl.semaphore_wait(barrier, n - 1)
            sends += [send(me, dev(h, False), i) for i, h in enumerate(hops)]
            sends.append(send(me, partner, len(hops)))
        else:
            rows += [best_of(me, (g - 1) * gran + k) for k in range(gran)]
    rows += [best_of(me, (n_gran - 1) * gran + k) for k in range(gran)]
    total = scores(me, rows)

    def forward(h, i):
        slot = dev(h, False)
        arrive(slot)
        sends.append(send(slot, partner, i))

    def blocks(slots):
        return functools.reduce(lambda x, y: x + y, [
            scores(slot, [best_of(slot, j) for j in range(pairs)]) for slot in slots])

    forward(hops[0], len(hops) + 1)
    forward(hops[1], len(hops) + 2)
    arrive(partner)
    total += blocks([partner] + [dev(h, False) for h in hops[:2]])
    for i, h in enumerate(hops[2:]):
        forward(h, len(hops) + 3 + i)
    for h in hops:
        arrive(dev(h, True))
    total += blocks([dev(h, True) for h in hops[:2]] + [dev(h, o) for h in hops[2:] for o in (False, True)])

    mine = pl.ds(pl.multiple_of(me * pairs, pairs), pairs)
    s_all[mine, :] = total
    s_sends = []
    for o in range(1, n):
        c = pltpu.make_async_remote_copy(
            src_ref=s_all.at[mine], dst_ref=s_all.at[mine], send_sem=s_send.at[o], recv_sem=s_recv.at[me],
            device_id={'data': lax.rem(me + o, n)}, device_id_type=MESH)
        c.start()
        s_sends.append(c)
    for c in sends:
        c.wait_send()
    for o in range(1, n):
        src = lax.rem(me + o, n)
        theirs = pl.ds(pl.multiple_of(src * pairs, pairs), pairs)
        pltpu.make_async_remote_copy(
            src_ref=s_all.at[theirs], dst_ref=s_all.at[theirs], send_sem=s_send.at[o], recv_sem=s_recv.at[src],
            device_id={'data': src}, device_id_type=MESH).wait_recv()
    for c in s_sends:
        c.wait_send()


def losses(pairs, s_ref, temp_ref, lq_ref, ld_ref, lm_ref):
    z = s_ref[...] / temp_ref[0]
    size = s_ref.shape[0]
    me = lax.axis_index('data')
    diag = (lax.broadcasted_iota(jnp.int32, (size, size), 0) == lax.broadcasted_iota(jnp.int32, (size, size), 1))
    pos_logit = jnp.sum(jnp.where(diag, z, 0.0), axis=0, keepdims=True)

    def lse(v):
        top = jnp.max(v, axis=0, keepdims=True)
        return jnp.log(jnp.sum(jnp.exp(v - top), axis=0, keepdims=True)) + top

    loss_q = lse(z) - pos_logit
    loss_d = lse(z.T) - pos_logit
    lm_ref[0] = jnp.sum(loss_q + loss_d) / (2 * size)
    back = lax.rem(size - me * pairs, size)
    lq_ref[...] = pltpu.roll(loss_q, back, 1)[:, :pairs]
    ld_ref[...] = pltpu.roll(loss_d, back, 1)[:, :pairs]


def solution(mesh):
    n = mesh.shape['data']
    batch_spec = P(('replica', 'data'))

    def local_loss(q_hidden, d_hidden, w_proj, q_mask, d_mask, temperature):
        pairs, q_len, hidden = q_hidden.shape
        d_len = d_hidden.shape[1]
        k = w_proj.shape[1]
        gran = 4
        any_ = pl.BlockSpec(memory_space=pl.ANY)
        vmem, smem = pl.BlockSpec(memory_space=pltpu.VMEM), pl.BlockSpec(memory_space=pltpu.SMEM)
        scores = pl.pallas_call(
            functools.partial(kernel, (n, pairs, q_len, d_len, gran)),
            out_shape=jax.ShapeDtypeStruct((n * pairs, n * pairs), jnp.float32),
            in_specs=[any_] * 5,
            out_specs=vmem,
            scratch_shapes=[
                pltpu.VMEM((hidden, k), jnp.bfloat16),
                pltpu.VMEM((pairs * q_len, hidden), jnp.bfloat16),
                pltpu.VMEM((pairs * d_len, hidden), jnp.bfloat16),
                pltpu.VMEM((pairs, q_len), jnp.int32),
                pltpu.VMEM((pairs, d_len), jnp.int32),
                pltpu.VMEM((n, k, pairs * q_len), jnp.bfloat16),
                pltpu.VMEM((pairs * d_len, k), jnp.bfloat16),
                pltpu.VMEM((d_len, pairs), jnp.float32),
                pltpu.SemaphoreType.DMA((4,)),
                pltpu.SemaphoreType.DMA((pairs // gran,)),
                pltpu.SemaphoreType.DMA((n,)),
                pltpu.SemaphoreType.DMA((n,)),
                pltpu.SemaphoreType.DMA((n,)),
                pltpu.SemaphoreType.DMA((n,)),
            ],
            compiler_params=pltpu.CompilerParams(
                collective_id=0, has_side_effects=True),
        )(q_hidden.reshape(pairs * q_len, hidden), d_hidden.reshape(pairs * d_len, hidden), w_proj,
          q_mask, d_mask)
        lq, ld, lm = pl.pallas_call(
            functools.partial(losses, pairs),
            out_shape=(jax.ShapeDtypeStruct((1, pairs), jnp.float32), jax.ShapeDtypeStruct((1, pairs), jnp.float32),
                       jax.ShapeDtypeStruct((1,), jnp.float32)),
            in_specs=[vmem, smem],
            out_specs=(vmem, vmem, smem),
        )(scores, temperature.reshape(1))
        return lq.reshape(pairs), ld.reshape(pairs), lm

    return jax.shard_map(local_loss, mesh=mesh, in_specs=(batch_spec, batch_spec, P(), batch_spec, batch_spec, P()),
                         out_specs=(batch_spec, batch_spec, P('replica')), check_vma=False)
```

```python
import functools
import jax
import jax.numpy as jnp
from jax import lax
from jax.experimental import pallas as pl
from jax.experimental.pallas import tpu as pltpu
from jax.sharding import PartitionSpec as P

MESH = pl.DeviceIdType.MESH


def unit_rows(x):
    return x * lax.rsqrt(jnp.sum(x * x, axis=1, keepdims=True))


def kernel(dims, q_hbm, d_hbm, w_hbm, qm_hbm, dm_hbm, s_all,
           w, qh, dh, qm, dm, qall, u, bias,
           in_sem, d_sem, q_send, q_recv, s_send, s_recv):
    n, pairs, q_len, d_len, gran = dims
    q_rows = pairs * q_len
    me = lax.axis_index('data')
    core = lax.rem(me, 2)
    chip = me // 2
    chips = n // 2
    partner = chip * 2 + (1 - core)

    def dev(dc, other):
        c = lax.rem(chip + dc, chips)
        return c * 2 + ((1 - core) if other else core)

    ins = [pltpu.make_async_copy(src, dst, in_sem.at[i]) for i, (src, dst) in enumerate(
        ((dm_hbm, dm), (qm_hbm, qm), (w_hbm, w), (q_hbm, qh)))]
    for c in ins:
        c.start()
    grows = gran * d_len
    n_gran = pairs // gran
    d_copies = []
    for g in range(n_gran):
        c = pltpu.make_async_copy(d_hbm.at[pl.ds(g * grows, grows)], dh.at[pl.ds(g * grows, grows)], d_sem.at[g])
        d_copies.append(c)
    for c in d_copies[:2]:
        c.start()

    barrier = pltpu.get_barrier_semaphore()
    for o in range(1, n):
        pl.semaphore_signal(barrier, inc=1, device_id={'data': lax.rem(me + o, n)}, device_id_type=MESH)

    for c in ins[:2]:
        c.wait()

    bias_t = jnp.where(dm[...] == 1, 0.0, -jnp.inf).T
    for j in range(pairs):
        bias[pl.ds(j * d_len, d_len), :] = jnp.broadcast_to(bias_t[:, j:j + 1], (d_len, 128))

    for c in ins[2:]:
        c.wait()

    def send(slot, target, i):
        c = pltpu.make_async_remote_copy(
            src_ref=qall.at[slot], dst_ref=qall.at[slot], send_sem=q_send.at[i], recv_sem=q_recv.at[slot],
            device_id={'data': target}, device_id_type=MESH)
        c.start()
        return c

    def arrive(slot):
        pltpu.make_async_remote_copy(
            src_ref=qall.at[slot], dst_ref=qall.at[slot], send_sem=q_send.at[0], recv_sem=q_recv.at[slot],
            device_id={'data': partner}, device_id_type=MESH).wait_recv()

    hops = [1, chips - 1] + list(range(2, chips - 1))
    sends = []

    def project_queries():
        row = lax.broadcasted_iota(jnp.int32, (q_rows, pairs), 0)
        own = (row // q_len == lax.broadcasted_iota(jnp.int32, (q_rows, pairs), 1)).astype(jnp.bfloat16)
        spread = jnp.dot(own, qm[...].astype(jnp.bfloat16), preferred_element_type=jnp.float32)
        row = lax.broadcasted_iota(jnp.int32, (q_rows, q_len), 0)
        tok = lax.broadcasted_iota(jnp.int32, (q_rows, q_len), 1)
        q_keep = jnp.sum(jnp.where(row % q_len == tok, spread, 0.0), axis=1, keepdims=True)
        xq = unit_rows(jnp.dot(qh[...], w[...], preferred_element_type=jnp.float32))
        qall[me] = jnp.where(q_keep > 0.5, xq, 0.0).T.astype(jnp.bfloat16)

    def project(g):
        here = pl.ds(g * grows, grows)
        x = jnp.dot(dh[here, :], w[...], preferred_element_type=jnp.float32)
        r = lax.rsqrt(jnp.sum(x * x, axis=1, keepdims=True))
        u[here, :] = (x * jnp.where(bias[here, :] == 0.0, r, 0.0)).astype(jnp.bfloat16)

    def best_of(slot, j):
        here = pl.ds(j * d_len, d_len)
        sim = jnp.dot(u[here, :], qall[slot], preferred_element_type=jnp.float32)
        return jnp.max(sim + jnp.concatenate([bias[here, :]] * (q_rows // 128), axis=1), axis=0, keepdims=True)

    sel = (lax.broadcasted_iota(jnp.int32, (q_rows, 128), 0) // q_len
           == lax.broadcasted_iota(jnp.int32, (q_rows, 128), 1)).astype(jnp.bfloat16)

    def scores(slot, rows):
        best = jnp.concatenate(rows, axis=0)
        hi = best.astype(jnp.bfloat16)
        r1 = best - hi.astype(jnp.float32)
        mid = r1.astype(jnp.bfloat16)
        lo = (r1 - mid.astype(jnp.float32)).astype(jnp.bfloat16)
        s = jnp.dot(hi, sel, preferred_element_type=jnp.float32)
        s = s + (jnp.dot(mid, sel, preferred_element_type=jnp.float32)
                 + jnp.dot(lo, sel, preferred_element_type=jnp.float32))
        return pltpu.roll(s, slot * pairs, 1)

    rows = []
    for g in range(n_gran):
        d_copies[g].wait()
        if g + 2 < n_gran:
            d_copies[g + 2].start()
        if g == 0:
            project_queries()
        project(g)
        if g == 0:
            pl.semaphore_wait(barrier, n - 1)
            sends += [send(me, dev(h, False), i) for i, h in enumerate(hops)]
            sends.append(send(me, partner, len(hops)))
        else:
            rows += [best_of(me, (g - 1) * gran + k) for k in range(gran)]
    rows += [best_of(me, (n_gran - 1) * gran + k) for k in range(gran)]
    total = scores(me, rows)

    def forward(h, i):
        slot = dev(h, False)
        arrive(slot)
        sends.append(send(slot, partner, i))

    def blocks(slots):
        return functools.reduce(lambda x, y: x + y, [
            scores(slot, [best_of(slot, j) for j in range(pairs)]) for slot in slots])

    for i, h in enumerate(hops[:2]):
        forward(h, len(hops) + 1 + i)
    arrive(partner)
    total += blocks([partner] + [dev(h, False) for h in hops[:2]])
    for i, h in enumerate(hops[2:]):
        forward(h, len(hops) + 3 + i)
    for h in hops[:2]:
        arrive(dev(h, True))
    total += blocks([dev(h, True) for h in hops[:2]])
    for h in hops[2:]:
        arrive(dev(h, True))
    total += blocks([dev(h, o) for h in hops[2:] for o in (False, True)])

    mine = pl.ds(pl.multiple_of(me * pairs, pairs), pairs)
    s_all[mine, :] = total
    s_sends = []
    for o in range(1, n):
        c = pltpu.make_async_remote_copy(
            src_ref=s_all.at[mine], dst_ref=s_all.at[mine], send_sem=s_send.at[o], recv_sem=s_recv.at[me],
            device_id={'data': lax.rem(me + o, n)}, device_id_type=MESH)
        c.start()
        s_sends.append(c)
    for c in sends:
        c.wait_send()
    for o in range(1, n):
        src = lax.rem(me + o, n)
        theirs = pl.ds(pl.multiple_of(src * pairs, pairs), pairs)
        pltpu.make_async_remote_copy(
            src_ref=s_all.at[theirs], dst_ref=s_all.at[theirs], send_sem=s_send.at[o], recv_sem=s_recv.at[src],
            device_id={'data': src}, device_id_type=MESH).wait_recv()
    for c in s_sends:
        c.wait_send()


def losses(pairs, s_ref, temp_ref, lq_ref, ld_ref, lm_ref):
    z = s_ref[...] / temp_ref[0]
    size = s_ref.shape[0]
    me = lax.axis_index('data')
    diag = (lax.broadcasted_iota(jnp.int32, (size, size), 0) == lax.broadcasted_iota(jnp.int32, (size, size), 1))
    pos_logit = jnp.sum(jnp.where(diag, z, 0.0), axis=0, keepdims=True)

    def lse(v):
        top = jnp.max(v, axis=0, keepdims=True)
        return jnp.log(jnp.sum(jnp.exp(v - top), axis=0, keepdims=True)) + top

    loss_q = lse(z) - pos_logit
    loss_d = lse(z.T) - pos_logit
    lm_ref[0] = jnp.sum(loss_q + loss_d) / (2 * size)
    back = lax.rem(size - me * pairs, size)
    lq_ref[...] = pltpu.roll(loss_q, back, 1)[:, :pairs]
    ld_ref[...] = pltpu.roll(loss_d, back, 1)[:, :pairs]


def solution(mesh):
    n = mesh.shape['data']
    batch_spec = P(('replica', 'data'))

    def local_loss(q_hidden, d_hidden, w_proj, q_mask, d_mask, temperature):
        pairs, q_len, hidden = q_hidden.shape
        d_len = d_hidden.shape[1]
        k = w_proj.shape[1]
        gran = 2
        hbm = pl.BlockSpec(memory_space=pltpu.HBM)
        vmem, smem = pl.BlockSpec(memory_space=pltpu.VMEM), pl.BlockSpec(memory_space=pltpu.SMEM)
        scores = pl.pallas_call(
            functools.partial(kernel, (n, pairs, q_len, d_len, gran)),
            out_shape=jax.ShapeDtypeStruct((n * pairs, n * pairs), jnp.float32),
            in_specs=[hbm] * 5,
            out_specs=vmem,
            scratch_shapes=[
                pltpu.VMEM((hidden, k), jnp.bfloat16),
                pltpu.VMEM((pairs * q_len, hidden), jnp.bfloat16),
                pltpu.VMEM((pairs * d_len, hidden), jnp.bfloat16),
                pltpu.VMEM((pairs, q_len), jnp.int32),
                pltpu.VMEM((pairs, d_len), jnp.int32),
                pltpu.VMEM((n, k, pairs * q_len), jnp.bfloat16),
                pltpu.VMEM((pairs * d_len, k), jnp.bfloat16),
                pltpu.VMEM((pairs * d_len, 128), jnp.float32),
                pltpu.SemaphoreType.DMA((4,)),
                pltpu.SemaphoreType.DMA((pairs // gran,)),
                pltpu.SemaphoreType.DMA((n,)),
                pltpu.SemaphoreType.DMA((n,)),
                pltpu.SemaphoreType.DMA((n,)),
                pltpu.SemaphoreType.DMA((n,)),
            ],
            compiler_params=pltpu.CompilerParams(
                collective_id=0, has_side_effects=True),
        )(q_hidden.reshape(pairs * q_len, hidden), d_hidden.reshape(pairs * d_len, hidden), w_proj,
          q_mask, d_mask)
        lq, ld, lm = pl.pallas_call(
            functools.partial(losses, pairs),
            out_shape=(jax.ShapeDtypeStruct((1, pairs), jnp.float32), jax.ShapeDtypeStruct((1, pairs), jnp.float32),
                       jax.ShapeDtypeStruct((1,), jnp.float32)),
            in_specs=[vmem, smem],
            out_specs=(vmem, vmem, smem),
        )(scores, temperature.reshape(1))
        return lq.reshape(pairs), ld.reshape(pairs), lm

    return jax.shard_map(local_loss, mesh=mesh, in_specs=(batch_spec, batch_spec, P(), batch_spec, batch_spec, P()),
                         out_specs=(batch_spec, batch_spec, P('replica')), check_vma=False)
```

```python
import functools
import jax
import jax.numpy as jnp
from jax import lax
from jax.experimental import pallas as pl
from jax.experimental.pallas import tpu as pltpu
from jax.sharding import PartitionSpec as P

MESH = pl.DeviceIdType.MESH


def unit_rows(x):
    return x * lax.rsqrt(jnp.sum(x * x, axis=1, keepdims=True))


def kernel(dims, q_hbm, d_hbm, w_hbm, qm_hbm, dm_hbm, s_all,
           w, qh, dh, qm, dm, qall, u, bias,
           in_sem, d_sem, q_send, q_recv, s_send, s_recv):
    n, pairs, q_len, d_len, gran = dims
    q_rows = pairs * q_len
    me = lax.axis_index('data')
    core = lax.rem(me, 2)
    chip = me // 2
    chips = n // 2
    partner = chip * 2 + (1 - core)

    def dev(dc, other):
        c = lax.rem(chip + dc, chips)
        return c * 2 + ((1 - core) if other else core)

    ins = [pltpu.make_async_copy(src, dst, in_sem.at[i]) for i, (src, dst) in enumerate(
        ((dm_hbm, dm), (qm_hbm, qm), (w_hbm, w), (q_hbm, qh)))]
    for c in ins:
        c.start()
    grows = gran * d_len
    n_gran = pairs // gran
    d_copies = []
    for g in range(n_gran):
        c = pltpu.make_async_copy(d_hbm.at[pl.ds(g * grows, grows)], dh.at[pl.ds(g * grows, grows)], d_sem.at[g])
        d_copies.append(c)
    for c in d_copies[:2]:
        c.start()

    barrier = pltpu.get_barrier_semaphore()
    for o in range(1, n):
        pl.semaphore_signal(barrier, inc=1, device_id={'data': lax.rem(me + o, n)}, device_id_type=MESH)

    for c in ins[:2]:
        c.wait()

    bias_t = jnp.where(dm[...] == 1, 0.0, -jnp.inf).T
    for j in range(pairs):
        bias[pl.ds(j * d_len, d_len), :] = jnp.broadcast_to(bias_t[:, j:j + 1], (d_len, 128))

    for c in ins[2:]:
        c.wait()

    def send(slot, target, i):
        c = pltpu.make_async_remote_copy(
            src_ref=qall.at[slot], dst_ref=qall.at[slot], send_sem=q_send.at[i], recv_sem=q_recv.at[slot],
            device_id={'data': target}, device_id_type=MESH)
        c.start()
        return c

    def arrive(slot):
        pltpu.make_async_remote_copy(
            src_ref=qall.at[slot], dst_ref=qall.at[slot], send_sem=q_send.at[0], recv_sem=q_recv.at[slot],
            device_id={'data': partner}, device_id_type=MESH).wait_recv()

    hops = [1, chips - 1] + list(range(2, chips - 1))
    sends = []

    def project_queries():
        row = lax.broadcasted_iota(jnp.int32, (q_rows, pairs), 0)
        own = (row // q_len == lax.broadcasted_iota(jnp.int32, (q_rows, pairs), 1)).astype(jnp.bfloat16)
        spread = jnp.dot(own, qm[...].astype(jnp.bfloat16), preferred_element_type=jnp.float32)
        row = lax.broadcasted_iota(jnp.int32, (q_rows, q_len), 0)
        tok = lax.broadcasted_iota(jnp.int32, (q_rows, q_len), 1)
        q_keep = jnp.sum(jnp.where(row % q_len == tok, spread, 0.0), axis=1, keepdims=True)
        xq = unit_rows(jnp.dot(qh[...], w[...], preferred_element_type=jnp.float32))
        qall[me] = jnp.where(q_keep > 0.5, xq, 0.0).T.astype(jnp.bfloat16)

    def project(g):
        here = pl.ds(g * grows, grows)
        x = jnp.dot(dh[here, :], w[...], preferred_element_type=jnp.float32)
        r = lax.rsqrt(jnp.sum(x * x, axis=1, keepdims=True))
        u[here, :] = (x * jnp.where(bias[here, :] == 0.0, r, 0.0)).astype(jnp.bfloat16)

    def best_of(slot, j):
        here = pl.ds(j * d_len, d_len)
        sim = jnp.dot(u[here, :], qall[slot], preferred_element_type=jnp.float32)
        return jnp.max(sim + jnp.concatenate([bias[here, :]] * (q_rows // 128), axis=1), axis=0, keepdims=True)

    sel = (lax.broadcasted_iota(jnp.int32, (q_rows, 128), 0) // q_len
           == lax.broadcasted_iota(jnp.int32, (q_rows, 128), 1)).astype(jnp.bfloat16)

    def scores(slots, rows):
        best = jnp.concatenate(rows, axis=0)
        hi = best.astype(jnp.bfloat16)
        r1 = best - hi.astype(jnp.float32)
        mid = r1.astype(jnp.bfloat16)
        lo = (r1 - mid.astype(jnp.float32)).astype(jnp.bfloat16)
        s = jnp.dot(jnp.concatenate([hi, mid, lo], axis=0), sel, preferred_element_type=jnp.float32)
        m = best.shape[0]
        s = s[:m] + (s[m:2 * m] + s[2 * m:])
        return functools.reduce(lambda x, y: x + y, [
            pltpu.roll(s[i * pairs:(i + 1) * pairs], slot * pairs, 1) for i, slot in enumerate(slots)])

    rows = []
    for g in range(n_gran):
        d_copies[g].wait()
        if g + 2 < n_gran:
            d_copies[g + 2].start()
        if g == 0:
            project_queries()
        project(g)
        if g == 0:
            pl.semaphore_wait(barrier, n - 1)
            sends += [send(me, dev(h, False), i) for i, h in enumerate(hops)]
            sends.append(send(me, partner, len(hops)))
        else:
            rows += [best_of(me, (g - 1) * gran + k) for k in range(gran)]
    rows += [best_of(me, (n_gran - 1) * gran + k) for k in range(gran)]
    total = scores([me], rows)

    def forward(h, i):
        slot = dev(h, False)
        arrive(slot)
        sends.append(send(slot, partner, i))

    def blocks(slots):
        return scores(slots, [best_of(slot, j) for slot in slots for j in range(pairs)])

    for i, h in enumerate(hops[:2]):
        forward(h, len(hops) + 1 + i)
    arrive(partner)
    total += blocks([partner] + [dev(h, False) for h in hops[:2]])
    for i, h in enumerate(hops[2:]):
        forward(h, len(hops) + 3 + i)
    for h in hops[:2]:
        arrive(dev(h, True))
    total += blocks([dev(h, True) for h in hops[:2]])
    for h in hops[2:]:
        arrive(dev(h, True))
    total += blocks([dev(h, o) for h in hops[2:] for o in (False, True)])

    mine = pl.ds(pl.multiple_of(me * pairs, pairs), pairs)
    s_all[mine, :] = total
    s_sends = []
    for o in sorted(range(1, n), key=lambda o: -min(o, n - o)):
        c = pltpu.make_async_remote_copy(
            src_ref=s_all.at[mine], dst_ref=s_all.at[mine], send_sem=s_send.at[o], recv_sem=s_recv.at[me],
            device_id={'data': lax.rem(me + o, n)}, device_id_type=MESH)
        c.start()
        s_sends.append(c)
    for c in sends:
        c.wait_send()
    for o in range(1, n):
        src = lax.rem(me + o, n)
        theirs = pl.ds(pl.multiple_of(src * pairs, pairs), pairs)
        pltpu.make_async_remote_copy(
            src_ref=s_all.at[theirs], dst_ref=s_all.at[theirs], send_sem=s_send.at[o], recv_sem=s_recv.at[src],
            device_id={'data': src}, device_id_type=MESH).wait_recv()
    for c in s_sends:
        c.wait_send()


def losses(pairs, s_ref, temp_ref, lq_ref, ld_ref, lm_ref):
    z = s_ref[...] / temp_ref[0]
    size = s_ref.shape[0]
    me = lax.axis_index('data')
    diag = (lax.broadcasted_iota(jnp.int32, (size, size), 0) == lax.broadcasted_iota(jnp.int32, (size, size), 1))
    pos_logit = jnp.sum(jnp.where(diag, z, 0.0), axis=0, keepdims=True)

    def lse(v):
        top = jnp.max(v, axis=0, keepdims=True)
        return jnp.log(jnp.sum(jnp.exp(v - top), axis=0, keepdims=True)) + top

    loss_q = lse(z) - pos_logit
    loss_d = lse(z.T) - pos_logit
    lm_ref[0] = jnp.sum(loss_q + loss_d) / (2 * size)
    back = lax.rem(size - me * pairs, size)
    lq_ref[...] = pltpu.roll(loss_q, back, 1)[:, :pairs]
    ld_ref[...] = pltpu.roll(loss_d, back, 1)[:, :pairs]


def solution(mesh):
    n = mesh.shape['data']
    batch_spec = P(('replica', 'data'))

    def local_loss(q_hidden, d_hidden, w_proj, q_mask, d_mask, temperature):
        pairs, q_len, hidden = q_hidden.shape
        d_len = d_hidden.shape[1]
        k = w_proj.shape[1]
        gran = 2
        hbm = pl.BlockSpec(memory_space=pltpu.HBM)
        vmem, smem = pl.BlockSpec(memory_space=pltpu.VMEM), pl.BlockSpec(memory_space=pltpu.SMEM)
        scores = pl.pallas_call(
            functools.partial(kernel, (n, pairs, q_len, d_len, gran)),
            out_shape=jax.ShapeDtypeStruct((n * pairs, n * pairs), jnp.float32),
            in_specs=[hbm] * 5,
            out_specs=vmem,
            scratch_shapes=[
                pltpu.VMEM((hidden, k), jnp.bfloat16),
                pltpu.VMEM((pairs * q_len, hidden), jnp.bfloat16),
                pltpu.VMEM((pairs * d_len, hidden), jnp.bfloat16),
                pltpu.VMEM((pairs, q_len), jnp.int32),
                pltpu.VMEM((pairs, d_len), jnp.int32),
                pltpu.VMEM((n, k, pairs * q_len), jnp.bfloat16),
                pltpu.VMEM((pairs * d_len, k), jnp.bfloat16),
                pltpu.VMEM((pairs * d_len, 128), jnp.float32),
                pltpu.SemaphoreType.DMA((4,)),
                pltpu.SemaphoreType.DMA((pairs // gran,)),
                pltpu.SemaphoreType.DMA((n,)),
                pltpu.SemaphoreType.DMA((n,)),
                pltpu.SemaphoreType.DMA((n,)),
                pltpu.SemaphoreType.DMA((n,)),
            ],
            compiler_params=pltpu.CompilerParams(
                collective_id=0, has_side_effects=True),
        )(q_hidden.reshape(pairs * q_len, hidden), d_hidden.reshape(pairs * d_len, hidden), w_proj,
          q_mask, d_mask)
        lq, ld, lm = pl.pallas_call(
            functools.partial(losses, pairs),
            out_shape=(jax.ShapeDtypeStruct((1, pairs), jnp.float32), jax.ShapeDtypeStruct((1, pairs), jnp.float32),
                       jax.ShapeDtypeStruct((1,), jnp.float32)),
            in_specs=[vmem, smem],
            out_specs=(vmem, vmem, smem),
        )(scores, temperature.reshape(1))
        return lq.reshape(pairs), ld.reshape(pairs), lm

    return jax.shard_map(local_loss, mesh=mesh, in_specs=(batch_spec, batch_spec, P(), batch_spec, batch_spec, P()),
                         out_specs=(batch_spec, batch_spec, P('replica')), check_vma=False)
```

```python
import functools
import jax
import jax.numpy as jnp
from jax import lax
from jax.experimental import pallas as pl
from jax.experimental.pallas import tpu as pltpu
from jax.sharding import PartitionSpec as P

MESH = pl.DeviceIdType.MESH
SCOPED = 60 * 1024 * 1024


def unit_rows(x):
    return x * lax.rsqrt(jnp.sum(x * x, axis=1, keepdims=True))


def kernel(dims, q_hbm, d_hbm, w_hbm, qm_hbm, dm_hbm, s_all,
           w, qh, dh, qm, dm, qall, u, bias,
           in_sem, d_sem, q_send, q_recv, s_send, s_recv):
    n, pairs, q_len, d_len, gran = dims
    q_rows = pairs * q_len
    me = lax.axis_index('data')
    core = lax.rem(me, 2)
    chip = me // 2
    chips = n // 2
    partner = chip * 2 + (1 - core)

    def dev(dc, other):
        c = lax.rem(chip + dc, chips)
        return c * 2 + ((1 - core) if other else core)

    ins = [pltpu.make_async_copy(src, dst, in_sem.at[i]) for i, (src, dst) in enumerate(
        ((dm_hbm, dm), (qm_hbm, qm), (w_hbm, w), (q_hbm, qh)))]
    for c in ins:
        c.start()
    grows = gran * d_len
    n_gran = pairs // gran
    d_copies = []
    for g in range(n_gran):
        c = pltpu.make_async_copy(d_hbm.at[pl.ds(g * grows, grows)], dh.at[pl.ds(g * grows, grows)], d_sem.at[g])
        d_copies.append(c)
    for c in d_copies[:2]:
        c.start()

    barrier = pltpu.get_barrier_semaphore()
    for o in range(1, n):
        pl.semaphore_signal(barrier, inc=1, device_id={'data': lax.rem(me + o, n)}, device_id_type=MESH)

    for c in ins[:2]:
        c.wait()

    bias_t = jnp.where(dm[...] == 1, 0.0, -jnp.inf).T
    for j in range(pairs):
        bias[pl.ds(j * d_len, d_len), :] = jnp.broadcast_to(bias_t[:, j:j + 1], (d_len, 128))

    for c in ins[2:]:
        c.wait()

    def send(slot, target, i):
        c = pltpu.make_async_remote_copy(
            src_ref=qall.at[slot], dst_ref=qall.at[slot], send_sem=q_send.at[i], recv_sem=q_recv.at[slot],
            device_id={'data': target}, device_id_type=MESH)
        c.start()
        return c

    def arrive(slot):
        pltpu.make_async_remote_copy(
            src_ref=qall.at[slot], dst_ref=qall.at[slot], send_sem=q_send.at[0], recv_sem=q_recv.at[slot],
            device_id={'data': partner}, device_id_type=MESH).wait_recv()

    hops = [1, chips - 1] + list(range(2, chips - 1))
    sends = []

    def project_queries():
        row = lax.broadcasted_iota(jnp.int32, (q_rows, pairs), 0)
        own = (row // q_len == lax.broadcasted_iota(jnp.int32, (q_rows, pairs), 1)).astype(jnp.bfloat16)
        spread = jnp.dot(own, qm[...].astype(jnp.bfloat16), preferred_element_type=jnp.float32)
        row = lax.broadcasted_iota(jnp.int32, (q_rows, q_len), 0)
        tok = lax.broadcasted_iota(jnp.int32, (q_rows, q_len), 1)
        q_keep = jnp.sum(jnp.where(row % q_len == tok, spread, 0.0), axis=1, keepdims=True)
        xq = unit_rows(jnp.dot(qh[...], w[...], preferred_element_type=jnp.float32))
        qall[me] = jnp.where(q_keep > 0.5, xq, 0.0).T.astype(jnp.bfloat16)

    def project(g):
        here = pl.ds(g * grows, grows)
        x = jnp.dot(dh[here, :], w[...], preferred_element_type=jnp.float32)
        r = lax.rsqrt(jnp.sum(x * x, axis=1, keepdims=True))
        u[here, :] = (x * jnp.where(bias[here, :] == 0.0, r, 0.0)).astype(jnp.bfloat16)

    def best_of(slot, j):
        here = pl.ds(j * d_len, d_len)
        sim = jnp.dot(u[here, :], qall[slot], preferred_element_type=jnp.float32)
        return jnp.max(sim + jnp.concatenate([bias[here, :]] * (q_rows // 128), axis=1), axis=0, keepdims=True)

    sel = (lax.broadcasted_iota(jnp.int32, (q_rows, 128), 0) // q_len
           == lax.broadcasted_iota(jnp.int32, (q_rows, 128), 1)).astype(jnp.bfloat16)

    def scores(slots, rows):
        best = jnp.concatenate(rows, axis=0)
        hi = best.astype(jnp.bfloat16)
        r1 = best - hi.astype(jnp.float32)
        mid = r1.astype(jnp.bfloat16)
        lo = (r1 - mid.astype(jnp.float32)).astype(jnp.bfloat16)
        s = jnp.dot(jnp.concatenate([hi, mid, lo], axis=0), sel, preferred_element_type=jnp.float32)
        m = best.shape[0]
        s = s[:m] + (s[m:2 * m] + s[2 * m:])
        return functools.reduce(lambda x, y: x + y, [
            pltpu.roll(s[i * pairs:(i + 1) * pairs], slot * pairs, 1) for i, slot in enumerate(slots)])

    rows = []
    for g in range(n_gran):
        d_copies[g].wait()
        if g + 2 < n_gran:
            d_copies[g + 2].start()
        if g == 0:
            project_queries()
        project(g)
        if g == 0:
            pl.semaphore_wait(barrier, n - 1)
            sends += [send(me, dev(h, False), i) for i, h in enumerate(hops)]
            sends.append(send(me, partner, len(hops)))
        else:
            rows += [best_of(me, (g - 1) * gran + k) for k in range(gran)]
    rows += [best_of(me, (n_gran - 1) * gran + k) for k in range(gran)]
    total = scores([me], rows)

    def forward(h, i):
        slot = dev(h, False)
        arrive(slot)
        sends.append(send(slot, partner, i))

    def blocks(slots):
        return scores(slots, [best_of(slot, j) for slot in slots for j in range(pairs)])

    for i, h in enumerate(hops[:2]):
        forward(h, len(hops) + 1 + i)
    arrive(partner)
    total += blocks([partner] + [dev(h, False) for h in hops[:2]])
    for i, h in enumerate(hops[2:]):
        forward(h, len(hops) + 3 + i)
    for h in hops[:2]:
        arrive(dev(h, True))
    total += blocks([dev(h, True) for h in hops[:2]])
    for h in hops[2:]:
        arrive(dev(h, True))
    total += blocks([dev(h, o) for h in hops[2:] for o in (False, True)])

    mine = pl.ds(pl.multiple_of(me * pairs, pairs), pairs)
    s_all[mine, :] = total
    s_sends = []
    for o in sorted(range(1, n), key=lambda o: -min(o, n - o)):
        c = pltpu.make_async_remote_copy(
            src_ref=s_all.at[mine], dst_ref=s_all.at[mine], send_sem=s_send.at[o], recv_sem=s_recv.at[me],
            device_id={'data': lax.rem(me + o, n)}, device_id_type=MESH)
        c.start()
        s_sends.append(c)
    for c in sends:
        c.wait_send()
    for o in range(1, n):
        src = lax.rem(me + o, n)
        theirs = pl.ds(pl.multiple_of(src * pairs, pairs), pairs)
        pltpu.make_async_remote_copy(
            src_ref=s_all.at[theirs], dst_ref=s_all.at[theirs], send_sem=s_send.at[o], recv_sem=s_recv.at[src],
            device_id={'data': src}, device_id_type=MESH).wait_recv()
    for c in s_sends:
        c.wait_send()


def losses(pairs, s_ref, temp_ref, lq_ref, ld_ref, lm_ref):
    z = s_ref[...] / temp_ref[0]
    size = s_ref.shape[0]
    me = lax.axis_index('data')
    diag = (lax.broadcasted_iota(jnp.int32, (size, size), 0) == lax.broadcasted_iota(jnp.int32, (size, size), 1))
    pos_logit = jnp.sum(jnp.where(diag, z, 0.0), axis=0, keepdims=True)

    def lse(v):
        top = jnp.max(v, axis=0, keepdims=True)
        return jnp.log(jnp.sum(jnp.exp(v - top), axis=0, keepdims=True)) + top

    loss_q = lse(z) - pos_logit
    loss_d = lse(z.T) - pos_logit
    lm_ref[0] = jnp.sum(loss_q + loss_d) / (2 * size)
    back = lax.rem(size - me * pairs, size)
    lq_ref[...] = pltpu.roll(loss_q, back, 1)[:, :pairs]
    ld_ref[...] = pltpu.roll(loss_d, back, 1)[:, :pairs]


def solution(mesh):
    n = mesh.shape['data']
    batch_spec = P(('replica', 'data'))

    def local_loss(q_hidden, d_hidden, w_proj, q_mask, d_mask, temperature):
        pairs, q_len, hidden = q_hidden.shape
        d_len = d_hidden.shape[1]
        k = w_proj.shape[1]
        gran = 2
        hbm = pl.BlockSpec(memory_space=pltpu.HBM)
        vmem, smem = pl.BlockSpec(memory_space=pltpu.VMEM), pl.BlockSpec(memory_space=pltpu.SMEM)
        scores = pl.pallas_call(
            functools.partial(kernel, (n, pairs, q_len, d_len, gran)),
            out_shape=pltpu.VMEM((n * pairs, n * pairs), jnp.float32),
            in_specs=[hbm] * 5,
            out_specs=vmem,
            scratch_shapes=[
                pltpu.VMEM((hidden, k), jnp.bfloat16),
                pltpu.VMEM((pairs * q_len, hidden), jnp.bfloat16),
                pltpu.VMEM((pairs * d_len, hidden), jnp.bfloat16),
                pltpu.VMEM((pairs, q_len), jnp.int32),
                pltpu.VMEM((pairs, d_len), jnp.int32),
                pltpu.VMEM((n, k, pairs * q_len), jnp.bfloat16),
                pltpu.VMEM((pairs * d_len, k), jnp.bfloat16),
                pltpu.VMEM((pairs * d_len, 128), jnp.float32),
                pltpu.SemaphoreType.DMA((4,)),
                pltpu.SemaphoreType.DMA((pairs // gran,)),
                pltpu.SemaphoreType.DMA((n,)),
                pltpu.SemaphoreType.DMA((n,)),
                pltpu.SemaphoreType.DMA((n,)),
                pltpu.SemaphoreType.DMA((n,)),
            ],
            compiler_params=pltpu.CompilerParams(
                collective_id=0, has_side_effects=True, vmem_limit_bytes=SCOPED - 80 * 1024),
        )(q_hidden.reshape(pairs * q_len, hidden), d_hidden.reshape(pairs * d_len, hidden), w_proj,
          q_mask, d_mask)
        lq, ld, lm = pl.pallas_call(
            functools.partial(losses, pairs),
            out_shape=(jax.ShapeDtypeStruct((1, pairs), jnp.float32), jax.ShapeDtypeStruct((1, pairs), jnp.float32),
                       jax.ShapeDtypeStruct((1,), jnp.float32)),
            in_specs=[vmem, smem],
            out_specs=(vmem, vmem, smem),
            compiler_params=pltpu.CompilerParams(vmem_limit_bytes=4 * 1024 * 1024),
        )(scores, temperature.reshape(1))
        return lq.reshape(pairs), ld.reshape(pairs), lm

    return jax.shard_map(local_loss, mesh=mesh, in_specs=(batch_spec, batch_spec, P(), batch_spec, batch_spec, P()),
                         out_specs=(batch_spec, batch_spec, P('replica')), check_vma=False)
```

```python
import functools
import jax
import jax.numpy as jnp
from jax import lax
from jax.experimental import pallas as pl
from jax.experimental.pallas import tpu as pltpu
from jax.sharding import PartitionSpec as P

MESH = pl.DeviceIdType.MESH
SCOPED = 60 * 1024 * 1024


def unit_rows(x):
    return x * lax.rsqrt(jnp.sum(x * x, axis=1, keepdims=True))


def kernel(dims, q_hbm, d_hbm, w_hbm, qm_hbm, dm_hbm, s_all,
           w, qh, dh, qm, dm, qall, u, bias,
           in_sem, d_sem, q_send, q_recv, s_send, s_recv):
    n, pairs, q_len, d_len, gran = dims
    q_rows = pairs * q_len
    me = lax.axis_index('data')
    core = lax.rem(me, 2)
    chip = me // 2
    chips = n // 2
    partner = chip * 2 + (1 - core)

    def dev(dc, other):
        c = lax.rem(chip + dc, chips)
        return c * 2 + ((1 - core) if other else core)

    ins = [pltpu.make_async_copy(src, dst, in_sem.at[i]) for i, (src, dst) in enumerate(
        ((dm_hbm, dm), (qm_hbm, qm), (w_hbm, w), (q_hbm, qh)))]
    for c in ins:
        c.start()
    grows = gran * d_len
    n_gran = pairs // gran
    d_copies = []
    for g in range(n_gran):
        c = pltpu.make_async_copy(d_hbm.at[pl.ds(g * grows, grows)], dh.at[pl.ds(g * grows, grows)], d_sem.at[g])
        d_copies.append(c)
    d_copies[0].start()

    barrier = pltpu.get_barrier_semaphore()
    for o in range(1, n):
        pl.semaphore_signal(barrier, inc=1, device_id={'data': lax.rem(me + o, n)}, device_id_type=MESH)

    for c in ins[:2]:
        c.wait()

    bias_t = jnp.where(dm[...] == 1, 0.0, -jnp.inf).T
    for j in range(pairs):
        bias[pl.ds(j * d_len, d_len), :] = jnp.broadcast_to(bias_t[:, j:j + 1], (d_len, 128))

    for c in ins[2:]:
        c.wait()
    d_copies[1].start()

    def send(slot, target, i):
        c = pltpu.make_async_remote_copy(
            src_ref=qall.at[slot], dst_ref=qall.at[slot], send_sem=q_send.at[i], recv_sem=q_recv.at[slot],
            device_id={'data': target}, device_id_type=MESH)
        c.start()
        return c

    def arrive(slot):
        pltpu.make_async_remote_copy(
            src_ref=qall.at[slot], dst_ref=qall.at[slot], send_sem=q_send.at[0], recv_sem=q_recv.at[slot],
            device_id={'data': partner}, device_id_type=MESH).wait_recv()

    hops = [1, chips - 1] + list(range(2, chips - 1))
    sends = []

    def project_queries():
        row = lax.broadcasted_iota(jnp.int32, (q_rows, pairs), 0)
        own = (row // q_len == lax.broadcasted_iota(jnp.int32, (q_rows, pairs), 1)).astype(jnp.bfloat16)
        spread = jnp.dot(own, qm[...].astype(jnp.bfloat16), preferred_element_type=jnp.float32)
        row = lax.broadcasted_iota(jnp.int32, (q_rows, q_len), 0)
        tok = lax.broadcasted_iota(jnp.int32, (q_rows, q_len), 1)
        q_keep = jnp.sum(jnp.where(row % q_len == tok, spread, 0.0), axis=1, keepdims=True)
        xq = unit_rows(jnp.dot(qh[...], w[...], preferred_element_type=jnp.float32))
        qall[me] = jnp.where(q_keep > 0.5, xq, 0.0).T.astype(jnp.bfloat16)

    def project(g):
        for k in range(gran):
            here = pl.ds(g * grows + k * d_len, d_len)
            x = jnp.dot(dh[here, :], w[...], preferred_element_type=jnp.float32)
            r = lax.rsqrt(jnp.sum(x * x, axis=1, keepdims=True))
            u[here, :] = (x * jnp.where(bias[here, :] == 0.0, r, 0.0)).astype(jnp.bfloat16)

    def best_of(slot, j):
        here = pl.ds(j * d_len, d_len)
        sim = jnp.dot(u[here, :], qall[slot], preferred_element_type=jnp.float32)
        return jnp.max(sim + jnp.concatenate([bias[here, :]] * (q_rows // 128), axis=1), axis=0, keepdims=True)

    sel = (lax.broadcasted_iota(jnp.int32, (q_rows, 128), 0) // q_len
           == lax.broadcasted_iota(jnp.int32, (q_rows, 128), 1)).astype(jnp.bfloat16)

    def scores(slots, rows):
        best = jnp.concatenate(rows, axis=0)
        hi = best.astype(jnp.bfloat16)
        r1 = best - hi.astype(jnp.float32)
        mid = r1.astype(jnp.bfloat16)
        lo = (r1 - mid.astype(jnp.float32)).astype(jnp.bfloat16)
        s = jnp.dot(jnp.concatenate([hi, mid, lo], axis=0), sel, preferred_element_type=jnp.float32)
        m = best.shape[0]
        s = s[:m] + (s[m:2 * m] + s[2 * m:])
        return functools.reduce(lambda x, y: x + y, [
            pltpu.roll(s[i * pairs:(i + 1) * pairs], slot * pairs, 1) for i, slot in enumerate(slots)])

    rows = []
    for g in range(n_gran):
        d_copies[g].wait()
        if g + 2 < n_gran:
            d_copies[g + 2].start()
        if g == 0:
            project_queries()
        project(g)
        if g == 0:
            pl.semaphore_wait(barrier, n - 1)
            sends += [send(me, dev(h, False), i) for i, h in enumerate(hops)]
            sends.append(send(me, partner, len(hops)))
        else:
            rows += [best_of(me, (g - 1) * gran + k) for k in range(gran)]
    rows += [best_of(me, (n_gran - 1) * gran + k) for k in range(gran)]
    total = scores([me], rows)

    def forward(h, i):
        slot = dev(h, False)
        arrive(slot)
        sends.append(send(slot, partner, i))

    def blocks(slots):
        return scores(slots, [best_of(slot, j) for slot in slots for j in range(pairs)])

    for i, h in enumerate(hops[:2]):
        forward(h, len(hops) + 1 + i)
    arrive(partner)
    total += blocks([partner] + [dev(h, False) for h in hops[:2]])
    for i, h in enumerate(hops[2:]):
        forward(h, len(hops) + 3 + i)
    for h in hops[:2]:
        arrive(dev(h, True))
    total += blocks([dev(h, True) for h in hops[:2]])
    for h in hops[2:]:
        arrive(dev(h, True))
    total += blocks([dev(h, o) for h in hops[2:] for o in (False, True)])

    mine = pl.ds(pl.multiple_of(me * pairs, pairs), pairs)
    s_all[mine, :] = total
    s_sends = []
    for o in sorted(range(1, n), key=lambda o: -min(o, n - o)):
        c = pltpu.make_async_remote_copy(
            src_ref=s_all.at[mine], dst_ref=s_all.at[mine], send_sem=s_send.at[o], recv_sem=s_recv.at[me],
            device_id={'data': lax.rem(me + o, n)}, device_id_type=MESH)
        c.start()
        s_sends.append(c)
    for c in sends:
        c.wait_send()
    for o in range(1, n):
        src = lax.rem(me + o, n)
        theirs = pl.ds(pl.multiple_of(src * pairs, pairs), pairs)
        pltpu.make_async_remote_copy(
            src_ref=s_all.at[theirs], dst_ref=s_all.at[theirs], send_sem=s_send.at[o], recv_sem=s_recv.at[src],
            device_id={'data': src}, device_id_type=MESH).wait_recv()
    for c in s_sends:
        c.wait_send()


def losses(pairs, s_ref, temp_ref, lq_ref, ld_ref, lm_ref):
    z = s_ref[...] / temp_ref[0]
    size = s_ref.shape[0]
    me = lax.axis_index('data')
    diag = (lax.broadcasted_iota(jnp.int32, (size, size), 0) == lax.broadcasted_iota(jnp.int32, (size, size), 1))
    pos_logit = jnp.sum(jnp.where(diag, z, 0.0), axis=0, keepdims=True)

    def lse(v):
        top = jnp.max(v, axis=0, keepdims=True)
        return jnp.log(jnp.sum(jnp.exp(v - top), axis=0, keepdims=True)) + top

    loss_q = lse(z) - pos_logit
    loss_d = lse(z.T) - pos_logit
    lm_ref[0] = jnp.sum(loss_q + loss_d) / (2 * size)
    back = lax.rem(size - me * pairs, size)
    lq_ref[...] = pltpu.roll(loss_q, back, 1)[:, :pairs]
    ld_ref[...] = pltpu.roll(loss_d, back, 1)[:, :pairs]


def solution(mesh):
    n = mesh.shape['data']
    batch_spec = P(('replica', 'data'))

    def local_loss(q_hidden, d_hidden, w_proj, q_mask, d_mask, temperature):
        pairs, q_len, hidden = q_hidden.shape
        d_len = d_hidden.shape[1]
        k = w_proj.shape[1]
        gran = 2
        hbm = pl.BlockSpec(memory_space=pltpu.HBM)
        vmem, smem = pl.BlockSpec(memory_space=pltpu.VMEM), pl.BlockSpec(memory_space=pltpu.SMEM)
        scores = pl.pallas_call(
            functools.partial(kernel, (n, pairs, q_len, d_len, gran)),
            out_shape=pltpu.VMEM((n * pairs, n * pairs), jnp.float32),
            in_specs=[hbm] * 5,
            out_specs=vmem,
            scratch_shapes=[
                pltpu.VMEM((hidden, k), jnp.bfloat16),
                pltpu.VMEM((pairs * q_len, hidden), jnp.bfloat16),
                pltpu.VMEM((pairs * d_len, hidden), jnp.bfloat16),
                pltpu.VMEM((pairs, q_len), jnp.int32),
                pltpu.VMEM((pairs, d_len), jnp.int32),
                pltpu.VMEM((n, k, pairs * q_len), jnp.bfloat16),
                pltpu.VMEM((pairs * d_len, k), jnp.bfloat16),
                pltpu.VMEM((pairs * d_len, 128), jnp.float32),
                pltpu.SemaphoreType.DMA((4,)),
                pltpu.SemaphoreType.DMA((pairs // gran,)),
                pltpu.SemaphoreType.DMA((n,)),
                pltpu.SemaphoreType.DMA((n,)),
                pltpu.SemaphoreType.DMA((n,)),
                pltpu.SemaphoreType.DMA((n,)),
            ],
            compiler_params=pltpu.CompilerParams(
                collective_id=0, has_side_effects=True, vmem_limit_bytes=SCOPED - 80 * 1024),
        )(q_hidden.reshape(pairs * q_len, hidden), d_hidden.reshape(pairs * d_len, hidden), w_proj,
          q_mask, d_mask)
        lq, ld, lm = pl.pallas_call(
            functools.partial(losses, pairs),
            out_shape=(jax.ShapeDtypeStruct((1, pairs), jnp.float32), jax.ShapeDtypeStruct((1, pairs), jnp.float32),
                       jax.ShapeDtypeStruct((1,), jnp.float32)),
            in_specs=[vmem, smem],
            out_specs=(vmem, vmem, smem),
            compiler_params=pltpu.CompilerParams(vmem_limit_bytes=4 * 1024 * 1024),
        )(scores, temperature.reshape(1))
        return lq.reshape(pairs), ld.reshape(pairs), lm

    return jax.shard_map(local_loss, mesh=mesh, in_specs=(batch_spec, batch_spec, P(), batch_spec, batch_spec, P()),
                         out_specs=(batch_spec, batch_spec, P('replica')), check_vma=False)
```
